32 devices in a mesh: cuts: 4 (over z), tile: 8 (over y, x, core).
Axes of the slice: x: 2, y: 2, z: 4, core: 2. Of those that a mesh axis runs over, the one named last changes fastest.
Arguments:
- probe_wave: float32 [2, 256, 256], replicated, may hold values from -6 to 6
- transmission: float32 [4, 2, 4096, 2048], P('cuts', None, None, 'tile'), may hold values from -1 to 1, as said below
- kernel_phase: float32 [256, 256], replicated, may hold values from -3.140625 to 3.140625
- measured: bfloat16 [8, 6, 256, 256], P('tile'), may hold values from 0 to 4
- counts: int32 [8], P('tile'), may hold values from 1 to 6, as said below
- positions: int32 [8, 6, 2], P('tile'), may hold values from 0 to 3840, as said below
- widths: int32 [8, 2], P('tile'), may hold values from 32 to 128
Outputs:
- adjoint_wave: float32 [4, 8, 6, 2, 256, 256], P('cuts', 'tile')
- object_grad: float32 [4, 2, 4096, 2048], P('cuts', None, None, 'tile')
The draws below stay inside these ranges and needn't reach their ends.
Inputs may be any that keep to these rules, and one draw needn't show every extreme that they name: Every entry has magnitude at most 1; each pair is a complex transmission. Tile t uses its first counts[t] slots; some tile uses all 6 slots. `positions`: rows lie in 0 to 3840 and columns in 0 to 256; column 0 of a tile's extended patch is 128 columns left of its first own column.
All inputs are finite; a program needn't handle non-finite values.
Results may differ from the reference program's by a relative error of at most 0.0003.
Values sent between devices are 32-bit elements; how exact they have to be, the bound alone decides.
A program may use at most 256 MiB of HBM per device.

```python
import math
import jax
import jax.numpy as jnp
from jax import lax

W = 256
TH = 4096
TW = 256
RIM = 128
CAP = 6
SLICES = 1
GROUPS = 4
TILES = 8
NCOL = 2048
NSLICE = 4


def draw_transmission(key, part):
    key_amp, key_phase = jax.random.split(key, 2)
    shape_here = (NSLICE, TH, NCOL)
    amplitude = jax.random.uniform(key_amp, shape_here, jnp.float32, 0.85, 1.0)
    phases = jnp.clip(0.6 * jax.random.normal(key_phase, shape_here, jnp.float32), -1.5, 1.5)
    return jnp.stack([amplitude * jnp.cos(phases), amplitude * jnp.sin(phases)], axis=1)


def draw_counts(key, part):
    key_light = jax.random.fold_in(key, 11)
    key_heavy = jax.random.fold_in(key, 12)
    key_pick = jax.random.fold_in(key, 13)
    light_load = jax.random.randint(key_light, (TILES,), 1, 4)
    heavy_load = jax.random.randint(key_heavy, (TILES,), 0, 4) == 0
    chosen = jax.random.randint(key_pick, (), 0, TILES)
    filled = heavy_load | (jnp.arange(TILES, dtype=jnp.int32) == chosen)
    return jnp.where(filled, CAP, light_load).astype(jnp.int32)


def draw_positions(key, part):
    key_rows = jax.random.fold_in(key, 21)
    key_cols = jax.random.fold_in(key, 22)
    row_place = jax.random.randint(key_rows, (TILES, CAP), 0, TH - W + 1)
    col_place = jax.random.randint(key_cols, (TILES, CAP), 0, TW + 2 * RIM - W + 1)
    return jnp.stack([row_place, col_place], axis=-1).astype(jnp.int32)


def set_ends(values, stream_key, smallest, top_value):
    dims = values.shape
    place = [jax.random.randint(jax.random.fold_in(stream_key, axis), (), 0, dims[axis]) for axis in range(len(dims))]
    values = values.at[tuple(place)].set(smallest)
    longest = dims.index(max(dims))
    place[longest] = (place[longest] + 1) % dims[longest]
    return values.at[tuple(place)].set(top_value)


def shard_levels(stream_key, dims, cuts, smallest, high):
    def one(axis_at, blocks):
        steps = jax.random.uniform(jax.random.fold_in(jax.random.fold_in(stream_key, 6), axis_at), (blocks,), jnp.float32, smallest / len(cuts), high / len(cuts))
        return jnp.repeat(jnp.exp(steps), dims[axis_at] // blocks).reshape((-1,) + (1,) * (len(dims) - axis_at - 1))

    level = one(*cuts[0])
    for cut in cuts[1:]:
        level = level * one(*cut)
    return level


def normal_values(rng, dims, width, reach, kind=jnp.bfloat16):
    values = width * jax.random.normal(rng, dims, jnp.float32)
    return jnp.clip(values, min=-reach, max=reach).astype(kind)


def setup_inputs(seed: int = 0) -> dict:
    key_of = jax.random.split(jax.random.key(seed), 8)
    return {
        "probe_wave": normal_values(key_of[0], (2, W, W), 1.0, 6.0, jnp.float32),
        "transmission": draw_transmission(jax.random.fold_in(key_of[7], 71), 0),
        "kernel_phase": jnp.clip(jax.random.uniform(key_of[2], (W, W), jnp.float32, -3.140625, 3.140625), -3.140625, 3.140625),
        "measured": jnp.clip(4.0 * jax.random.uniform(key_of[3], (TILES, CAP, W, W), jnp.float32) ** shard_levels(key_of[3], (TILES, CAP, W, W), ((0, 8),), -0.2, 0.2), 0.0, 4.0).astype(jnp.bfloat16),
        "counts": draw_counts(jax.random.fold_in(key_of[7], 71), 0),
        "positions": draw_positions(jax.random.fold_in(key_of[7], 71), 0),
        "widths": set_ends(jax.random.randint(key_of[6], (TILES, 2), RIM // 4, RIM + 1), jax.random.fold_in(key_of[6], 1), RIM // 4, RIM).astype(jnp.int32),
    }


def make_tables():
    indices = jnp.arange(W, dtype=jnp.int32)
    product = indices[:, None] * indices[None, :] % W
    angles = product.astype(jnp.float32) * (2.0 * math.pi / W)
    cosine = jnp.cos(angles) / math.sqrt(W)
    sine_part = jnp.sin(angles) / math.sqrt(W)
    forward = jnp.concatenate([jnp.concatenate([cosine, sine_part], 1), jnp.concatenate([-sine_part, cosine], 1)], 0)
    inverse = jnp.concatenate([jnp.concatenate([cosine, -sine_part], 1), jnp.concatenate([sine_part, cosine], 1)], 0)
    return (forward, inverse)

def transform(fields, matrix):
    number = fields.shape[0]
    stacked = fields.reshape(number, 2 * W, W)
    halfway = jnp.einsum('ab,pbc->pac', matrix, stacked, precision=lax.Precision.HIGHEST)
    halfway = halfway.reshape(number, 2, W, W)
    quadrant = matrix.reshape(2, W, 2, W)
    return jnp.einsum('psik,rjsk->prij', halfway, quadrant, precision=lax.Precision.HIGHEST)

def complex_mul(first_op, second_op):
    first_re, first_im = (first_op[..., 0, :, :], first_op[..., 1, :, :])
    second_re, second_im = (second_op[..., 0, :, :], second_op[..., 1, :, :])
    return jnp.stack([first_re * second_re - first_im * second_im, first_re * second_im + first_im * second_re], axis=-3)

def conj_mul(first_op, second_op):
    first_re, first_im = (first_op[..., 0, :, :], first_op[..., 1, :, :])
    second_re, second_im = (second_op[..., 0, :, :], second_op[..., 1, :, :])
    return jnp.stack([first_re * second_re + first_im * second_im, first_re * second_im - first_im * second_re], axis=-3)

def propagate(fields, kernel, tables):
    spectrum = transform(fields, tables[0])
    return transform(complex_mul(kernel, spectrum), tables[1])

def keep_columns(tile_at, width_pair):
    columns = jnp.arange(TW + 2 * RIM, dtype=jnp.int32)
    globally = tile_at * TW - RIM + columns
    inside = (globally >= 0) & (globally < TILES * TW)
    middle = (columns >= RIM) & (columns < RIM + TW)
    left_ok = (columns < RIM) & (RIM - columns <= width_pair[0])
    right_ok = (columns >= RIM + TW) & (columns - RIM - TW + 1 <= width_pair[1])
    return inside & (middle | left_ok | right_ok)

def cut_windows(grad_plane, places):
    anchor = jnp.zeros((), jnp.int32)

    def single(corner):
        return lax.dynamic_slice(grad_plane, (anchor, corner[0], corner[1]), (2, W, W))
    return jax.vmap(single)(places)

def add_windows(grad_plane, places, contrib):
    anchor = jnp.zeros((), jnp.int32)
    for item_at in range(contrib.shape[0]):
        corner_at = (anchor, places[item_at, 0], places[item_at, 1])
        current = lax.dynamic_slice(grad_plane, corner_at, (2, W, W))
        grad_plane = lax.dynamic_update_slice(grad_plane, current + contrib[item_at], corner_at)
    return grad_plane

def reference(probe_wave, transmission, kernel_phase, measured, counts, positions, widths):
    tables = make_tables()
    kernel = jnp.stack([jnp.cos(kernel_phase), jnp.sin(kernel_phase)], 0)
    kernel_conj = jnp.stack([jnp.cos(kernel_phase), -jnp.sin(kernel_phase)], 0)
    padded = jnp.pad(transmission, ((0, 0), (0, 0), (0, 0), (RIM, RIM)))
    vacuum = jnp.array([1.0, 0.0], dtype=jnp.float32)[:, None, None]

    def one_tile(operands):
        tile_at, count_here, places, width_pair, observed = operands
        keep_mask = keep_columns(tile_at, width_pair)
        object_patch = lax.dynamic_slice_in_dim(padded, tile_at * TW, TW + 2 * RIM, 3)
        object_patch = jnp.where(keep_mask, object_patch, vacuum)
        live_slots = (jnp.arange(CAP, dtype=jnp.int32) < count_here).astype(jnp.float32)
        fields = probe_wave[None] * live_slots[:, None, None, None]
        saved_waves = []
        window_list = []
        for slice_at in range(NSLICE):
            windows = cut_windows(object_patch[slice_at], places)
            saved_waves.append(fields)
            window_list.append(windows)
            fields = propagate(complex_mul(windows, fields), kernel, tables)
        far_field = transform(fields, tables[0])
        intensity = far_field[:, 0] * far_field[:, 0] + far_field[:, 1] * far_field[:, 1]
        residual = intensity - observed.astype(jnp.float32)
        backward = transform(far_field * residual[:, None], tables[1])
        grad_list = []
        entry_list = [None] * GROUPS
        for slice_at in reversed(range(NSLICE)):
            turned = propagate(backward, kernel_conj, tables)
            contrib = conj_mul(saved_waves[slice_at], turned)
            grad_plane = add_windows(jnp.zeros_like(object_patch[slice_at]), places, contrib)
            grad_list.insert(0, jnp.where(keep_mask, grad_plane, 0.0))
            backward = conj_mul(window_list[slice_at], turned)
            if slice_at % SLICES == 0:
                entry_list[slice_at // SLICES] = backward
        grad_patch = jnp.stack(grad_list, 0)
        return (jnp.stack(entry_list, 0), grad_patch[..., :RIM], grad_patch[..., RIM:RIM + TW], grad_patch[..., RIM + TW:])
    tile_ids = jnp.arange(TILES, dtype=jnp.int32)
    entries, left_rims, center, right_rims = lax.map(one_tile, (tile_ids, counts, positions, widths, measured))
    from_left = jnp.concatenate([jnp.zeros_like(right_rims[:1]), right_rims[:-1]], 0)
    from_right = jnp.concatenate([left_rims[1:], jnp.zeros_like(left_rims[:1])], 0)
    center = center.at[..., :RIM].add(from_left)
    center = center.at[..., TW - RIM:].add(from_right)
    object_grad = jnp.moveaxis(center, 0, 3).reshape(NSLICE, 2, TH, NCOL)
    adjoint_wave = jnp.swapaxes(entries, 0, 1)
    return (adjoint_wave, object_grad)
```

```python
import functools
import math

import jax
import jax.numpy as jnp
from jax import lax
from jax.experimental import pallas as pl
from jax.experimental.pallas import tpu as pltpu
from jax.sharding import PartitionSpec as P

RIM = 128
PAD = 8
MESH = pl.DeviceIdType.MESH
VMEM_LIMIT = 60 * 1024 * 1024


def params(**kw):
    return pltpu.CompilerParams(vmem_limit_bytes=VMEM_LIMIT, **kw)


def vmem():
    return pl.BlockSpec(memory_space=pltpu.VMEM)


def smem():
    return pl.BlockSpec(memory_space=pltpu.SMEM)


def shift(value, axis, by):
    count = lax.axis_size(axis)
    pairs = [(i, i + by) for i in range(count) if 0 <= i + by < count]
    return lax.ppermute(value, axis, pairs)


def make_tables(extent):
    indices = jnp.arange(extent, dtype=jnp.int32)
    product = indices[:, None] * indices[None, :] % extent
    angles = product.astype(jnp.float32) * (2.0 * math.pi / extent)
    cosine = jnp.cos(angles) / math.sqrt(extent)
    sine = jnp.sin(angles) / math.sqrt(extent)

    def split(x):
        hi = lax.reduce_precision(x, 8, 7)
        lo = x - hi
        return hi.astype(jnp.bfloat16), lo.astype(jnp.bfloat16)

    def square(c, s, sign):
        return jnp.concatenate(
            [jnp.concatenate([c, sign * s], 1), jnp.concatenate([-sign * s, c], 1)], 0
        )

    (ch, cl), (sh, sl) = split(cosine), split(sine)
    return (square(ch, sh, 1), square(cl, sl, 1), square(ch, sh, -1), square(cl, sl, -1))


def aligned(row, limit):
    base = jnp.minimum(row // PAD * PAD, limit)
    return pl.multiple_of(base, PAD), row - base


def extract_kernel(own_pos, left_pos, right_pos, trans, own, to_left, to_right,
                   buf_own, buf_left, buf_right, sems):
    slots, _, extent, cols = own.shape
    rows = trans.shape[1]
    tall = extent + PAD
    jobs = (
        (left_pos, buf_left, to_left, 0, RIM),
        (right_pos, buf_right, to_right, cols - RIM, RIM),
        (own_pos, buf_own, own, 0, cols),
    )

    def copy(j, s):
        pos, buf, _, start, width = jobs[j]
        base, off = aligned(pos[s, 0], rows - tall)
        src = trans.at[:, pl.ds(base, tall), pl.ds(start, width)]
        return pltpu.make_async_copy(src, buf.at[s], sems.at[j, s]), off

    for j in range(3):
        for s in range(slots):
            copy(j, s)[0].start()
    for j in range(3):
        _, buf, out, _, _ = jobs[j]

        def body(s, carry):
            one, off = copy(j, s)
            one.wait()
            for p in range(2):
                value = pltpu.roll(buf[s, p], (tall - off) % tall, 0)
                out[s, p] = value[:extent]
            return carry

        lax.fori_loop(0, slots, body, 0)


def keep_columns(shape, tile_at, tiles_total, widths, cols):
    columns = lax.broadcasted_iota(jnp.int32, shape, 1)
    globally = tile_at * cols - RIM + columns
    inside = (globally >= 0) & (globally < tiles_total * cols)
    middle = (columns >= RIM) & (columns < RIM + cols)
    left_ok = (columns < RIM) & (RIM - columns <= widths[0])
    right_ok = (columns >= RIM + cols) & (columns - RIM - cols + 1 <= widths[1])
    return inside & (middle | left_ok | right_ok)


def window_kernel(tiles_total, info, own_pos, left, own, right, out):
    extent, cols = own.shape[-2:]
    wide = cols + 2 * RIM
    s = pl.program_id(0)
    keep = keep_columns((extent, wide), info[2], tiles_total, (info[0], info[1]), cols)
    turn = (wide - own_pos[s, 1]) % wide
    for p in range(2):
        value = jnp.concatenate([left[0, p], own[0, p], right[0, p]], axis=1)
        value = jnp.where(keep, value, 1.0 - p)
        out[0, p] = pltpu.roll(value, turn, 1)[:, :extent]


def unwindow_kernel(tiles_total, info, own_pos, contrib, left, own, right):
    extent, cols = own.shape[-2:]
    wide = cols + 2 * RIM
    s = pl.program_id(0)
    keep = keep_columns((extent, wide), info[2], tiles_total, (info[0], info[1]), cols)
    for p in range(2):
        value = contrib[0, p]
        zeros = jnp.zeros((extent, wide - extent), jnp.float32)
        value = jnp.concatenate([value, zeros], axis=1)
        value = jnp.where(keep, pltpu.roll(value, own_pos[s, 1], 1), 0.0)
        left[0, p] = value[:, :RIM]
        own[0, p] = value[:, RIM : RIM + cols]
        right[0, p] = value[:, RIM + cols :]


def add_rows(out, pos, source, start, width):
    slots, _, extent, _ = source.shape
    rows = out.shape[1]
    tall = extent + PAD

    def body(s, carry):
        base, off = aligned(pos[s, 0], rows - tall)
        for p in range(2):
            value = jnp.concatenate([source[s, p], jnp.zeros((PAD, width), jnp.float32)], axis=0)
            value = pltpu.roll(value, off, 0)
            out[p, pl.ds(base, tall), pl.ds(start, width)] += value
        return carry

    lax.fori_loop(0, slots, body, 0)


def own_grad_kernel(own_pos, own, out):
    out[...] = jnp.zeros(out.shape, out.dtype)
    add_rows(out, own_pos, own, 0, out.shape[2])


def rim_grad_kernel(left_pos, right_pos, from_left, from_right, before, out):
    cols = out.shape[2]
    out[...] = before[...]
    add_rows(out, left_pos, from_left, 0, RIM)
    add_rows(out, right_pos, from_right, cols - RIM, RIM)


def pipeline_kernel(sections, live, windows, probe, phase_kernel, measured,
                    fwd_hi, fwd_lo, inv_hi, inv_lo, adjoint, contrib,
                    arrived, leaving, backed, leaving_back, left_f, left_i, right_f, right_i,
                    tall_b, wide_b, spectrum, send_f, recv_f, send_b, recv_b):
    g = lax.axis_index("cuts")
    last = sections - 1
    slots, _, extent, _ = windows.shape
    two = 2 * extent

    barrier = pltpu.get_barrier_semaphore()

    @pl.when(g > 0)
    def _():
        pl.semaphore_signal(barrier, inc=1, device_id={"cuts": g - 1}, device_id_type=MESH)

    @pl.when(g < last)
    def _():
        pl.semaphore_signal(barrier, inc=1, device_id={"cuts": g + 1}, device_id_type=MESH)

    for table, hi, lo in ((left_f, fwd_hi, fwd_lo), (left_i, inv_hi, inv_lo)):
        table[:, :two] = hi[...]
        table[:, two : 2 * two] = hi[...]
        table[:, 2 * two :] = lo[...]
    for table, hi, lo in ((right_f, inv_hi, inv_lo), (right_i, fwd_hi, fwd_lo)):
        table[:two] = hi[...]
        table[two : 2 * two] = hi[...]
        table[2 * two :] = lo[...]

    inner = (g > 0) & (g < last)

    @pl.when(inner)
    def _():
        pl.semaphore_wait(barrier, 2)

    @pl.when(jnp.logical_not(inner))
    def _():
        pl.semaphore_wait(barrier, 1)

    def put(ref, rows, p, value):
        hi = value.astype(jnp.bfloat16)
        lo = (value - hi.astype(jnp.float32)).astype(jnp.bfloat16)
        n = value.shape[0 if rows else 1]
        for at, part in ((0, hi), (1, lo), (2, hi)):
            place = pl.ds(at * two + p * n, n)
            if rows:
                ref[place, :] = part
            else:
                ref[:, place] = part

    def transform(left, right):
        half = jnp.dot(left[...], tall_b[...], preferred_element_type=jnp.float32)
        put(wide_b, False, 0, half[:extent])
        put(wide_b, False, 1, half[extent:])
        spectrum[...] = jnp.dot(wide_b[...], right[...], preferred_element_type=jnp.float32)

    def times_kernel(sign):
        kr, ki = phase_kernel[0], sign * phase_kernel[1]
        xr, xi = spectrum[:, :extent], spectrum[:, extent:]
        put(tall_b, True, 0, kr * xr - ki * xi)
        put(tall_b, True, 1, kr * xi + ki * xr)

    def propagate(sign):
        transform(left_f, right_f)
        times_kernel(sign)
        transform(left_i, right_i)

    def send_forward(s):
        return pltpu.make_async_remote_copy(
            src_ref=leaving.at[s], dst_ref=arrived.at[s], send_sem=send_f.at[s],
            recv_sem=recv_f.at[s], device_id={"cuts": g + 1}, device_id_type=MESH)

    def send_backward(s):
        return pltpu.make_async_remote_copy(
            src_ref=leaving_back.at[s], dst_ref=backed.at[s], send_sem=send_b.at[s],
            recv_sem=recv_b.at[s], device_id={"cuts": g - 1}, device_id_type=MESH)

    def forward(s):
        @pl.when(g == 0)
        def _():
            arrived[s] = probe[...] * live[s]

        @pl.when(g > 0)
        def _():
            send_forward(s).wait_recv()

        wr, wi = windows[s, 0], windows[s, 1]
        xr, xi = arrived[s, 0], arrived[s, 1]
        put(tall_b, True, 0, wr * xr - wi * xi)
        put(tall_b, True, 1, wr * xi + wi * xr)
        propagate(1.0)

        @pl.when(g < last)
        def _():
            leaving[s, 0] = spectrum[:, :extent]
            leaving[s, 1] = spectrum[:, extent:]
            send_forward(s).start()

    def backward(s):
        @pl.when(g == last)
        def _():
            put(tall_b, True, 0, spectrum[:, :extent])
            put(tall_b, True, 1, spectrum[:, extent:])
            transform(left_f, right_f)
            fr, fi = spectrum[:, :extent], spectrum[:, extent:]
            residual = fr * fr + fi * fi - measured[s].astype(jnp.float32)
            put(tall_b, True, 0, fr * residual)
            put(tall_b, True, 1, fi * residual)
            transform(left_i, right_i)
            put(tall_b, True, 0, spectrum[:, :extent])
            put(tall_b, True, 1, spectrum[:, extent:])

        @pl.when(g < last)
        def _():
            send_backward(s).wait_recv()
            put(tall_b, True, 0, backed[s, 0])
            put(tall_b, True, 1, backed[s, 1])

        propagate(-1.0)
        tr, ti = spectrum[:, :extent], spectrum[:, extent:]
        wr, wi = windows[s, 0], windows[s, 1]
        br, bi = wr * tr + wi * ti, wr * ti - wi * tr

        @pl.when(g > 0)
        def _():
            leaving_back[s, 0] = br
            leaving_back[s, 1] = bi
            send_backward(s).start()

        adjoint[s, 0] = br
        adjoint[s, 1] = bi
        xr, xi = arrived[s, 0], arrived[s, 1]
        contrib[s, 0] = xr * tr + xi * ti
        contrib[s, 1] = xr * ti - xi * tr

    lag = 2 * (last - g)

    def step(k, carry):
        @pl.when(k < slots)
        def _():
            forward(k)

        @pl.when((k >= lag) & (k < lag + slots))
        def _():
            backward(k - lag)

        return carry

    lax.fori_loop(0, slots + 2 * last, step, 0)

    @pl.when(g < last)
    def _():
        lax.fori_loop(0, slots, lambda s, c: (send_forward(s).wait_send(), c)[1], 0)

    @pl.when(g > 0)
    def _():
        lax.fori_loop(0, slots, lambda s, c: (send_backward(s).wait_send(), c)[1], 0)


def on_device(probe_wave, transmission, kernel_phase, measured, counts, positions, widths):
    f32 = jnp.float32
    rows, cols = transmission.shape[2:]
    extent = probe_wave.shape[-1]
    slots = positions.shape[1]
    sections = lax.axis_size("cuts")
    tiles_total = lax.axis_size("tile")
    tile_at = lax.axis_index("tile")
    tall = extent + PAD
    trans = transmission[0]
    own_pos = positions[0]
    right_pos = shift(own_pos, "tile", -1)
    left_pos = shift(own_pos, "tile", 1)
    info = jnp.concatenate([widths[0], tile_at[None].astype(jnp.int32)])
    sds = jax.ShapeDtypeStruct
    wave = sds((slots, 2, extent, extent), f32)
    block = sds((slots, 2, extent, cols), f32)
    rim = sds((slots, 2, extent, RIM), f32)

    own, to_left, to_right = pl.pallas_call(
        extract_kernel,
        out_shape=(block, rim, rim),
        in_specs=[smem(), smem(), smem(), pl.BlockSpec(memory_space=pl.ANY)],
        out_specs=(vmem(), vmem(), vmem()),
        scratch_shapes=[
            pltpu.VMEM((slots, 2, tall, cols), f32),
            pltpu.VMEM((slots, 2, tall, RIM), f32),
            pltpu.VMEM((slots, 2, tall, RIM), f32),
            pltpu.SemaphoreType.DMA((3, slots)),
        ],
        compiler_params=params(),
    )(own_pos, left_pos, right_pos, trans)
    right_rim = shift(to_left, "tile", -1)
    left_rim = shift(to_right, "tile", 1)

    def per_slot(width, height=extent):
        return pl.BlockSpec((1, 2, height, width), lambda s: (s, 0, 0, 0))

    windows = pl.pallas_call(
        functools.partial(window_kernel, tiles_total),
        grid=(slots,),
        out_shape=wave,
        in_specs=[smem(), smem(), per_slot(RIM), per_slot(cols), per_slot(RIM)],
        out_specs=per_slot(extent),
        compiler_params=params(),
    )(info, own_pos, left_rim, own, right_rim)

    tables = make_tables(extent)
    phase_kernel = jnp.stack([jnp.cos(kernel_phase), jnp.sin(kernel_phase)], 0)
    live = (jnp.arange(slots, dtype=jnp.int32) < counts[0]).astype(f32)
    waves = pltpu.VMEM((slots, 2, extent, extent), f32)
    two = 2 * extent
    bf16 = jnp.bfloat16
    adjoint, contrib = pl.pallas_call(
        functools.partial(pipeline_kernel, sections),
        out_shape=(wave, wave),
        in_specs=[smem()] + [vmem()] * 8,
        out_specs=(vmem(), vmem()),
        scratch_shapes=[
            waves, waves, waves, waves,
            pltpu.VMEM((two, 3 * two), bf16),
            pltpu.VMEM((two, 3 * two), bf16),
            pltpu.VMEM((3 * two, two), bf16),
            pltpu.VMEM((3 * two, two), bf16),
            pltpu.VMEM((3 * two, extent), bf16),
            pltpu.VMEM((extent, 3 * two), bf16),
            pltpu.VMEM((extent, two), f32),
            pltpu.SemaphoreType.DMA((slots,)),
            pltpu.SemaphoreType.DMA((slots,)),
            pltpu.SemaphoreType.DMA((slots,)),
            pltpu.SemaphoreType.DMA((slots,)),
        ],
        compiler_params=params(collective_id=0, has_side_effects=True),
    )(live, windows, probe_wave, phase_kernel, measured[0], *tables)

    left_part, own_part, right_part = pl.pallas_call(
        functools.partial(unwindow_kernel, tiles_total),
        grid=(slots,),
        out_shape=(rim, block, rim),
        in_specs=[smem(), smem(), per_slot(extent)],
        out_specs=(per_slot(RIM), per_slot(cols), per_slot(RIM)),
        compiler_params=params(),
    )(info, own_pos, contrib)
    from_right = shift(left_part, "tile", -1)
    from_left = shift(right_part, "tile", 1)
    plane = sds((2, rows, cols), f32)
    grad = pl.pallas_call(
        own_grad_kernel,
        out_shape=plane,
        in_specs=[smem(), vmem()],
        out_specs=vmem(),
        compiler_params=params(),
    )(own_pos, own_part)
    grad = pl.pallas_call(
        rim_grad_kernel,
        out_shape=plane,
        in_specs=[smem(), smem(), vmem(), vmem(), vmem()],
        out_specs=vmem(),
        compiler_params=params(),
    )(left_pos, right_pos, from_left, from_right, grad)
    return (adjoint[None, None], grad[None])


def solution(mesh):
    return jax.shard_map(
        on_device,
        mesh=mesh,
        in_specs=(
            P(),
            P("cuts", None, None, "tile"),
            P(),
            P("tile", None, None, None),
            P("tile"),
            P("tile", None, None),
            P("tile", None),
        ),
        out_specs=(P("cuts", "tile", None, None, None, None), P("cuts", None, None, "tile")),
        check_vma=False,
    )
```

```python
import functools
import math

import jax
import jax.numpy as jnp
from jax import lax
from jax.experimental import pallas as pl
from jax.experimental.pallas import tpu as pltpu
from jax.sharding import PartitionSpec as P

RIM = 128
PAD = 8
MESH = pl.DeviceIdType.MESH
VMEM_LIMIT = 60 * 1024 * 1024


def params(**kw):
    return pltpu.CompilerParams(vmem_limit_bytes=VMEM_LIMIT, **kw)


def vmem():
    return pl.BlockSpec(memory_space=pltpu.VMEM)


def smem():
    return pl.BlockSpec(memory_space=pltpu.SMEM)


def shift(value, axis, by):
    count = lax.axis_size(axis)
    pairs = [(i, i + by) for i in range(count) if 0 <= i + by < count]
    return lax.ppermute(value, axis, pairs)


def make_tables(extent):
    indices = jnp.arange(extent, dtype=jnp.int32)
    product = indices[:, None] * indices[None, :] % extent
    angles = product.astype(jnp.float32) * (2.0 * math.pi / extent)
    cosine = jnp.cos(angles) / math.sqrt(extent)
    sine = jnp.sin(angles) / math.sqrt(extent)

    def split(x):
        hi = lax.reduce_precision(x, 8, 7)
        lo = x - hi
        return hi.astype(jnp.bfloat16), lo.astype(jnp.bfloat16)

    def square(c, s, sign):
        return jnp.concatenate(
            [jnp.concatenate([c, sign * s], 1), jnp.concatenate([-sign * s, c], 1)], 0
        )

    (ch, cl), (sh, sl) = split(cosine), split(sine)
    return (square(ch, sh, 1), square(cl, sl, 1), square(ch, sh, -1), square(cl, sl, -1))


def aligned(row, limit):
    base = jnp.minimum(row // PAD * PAD, limit)
    return pl.multiple_of(base, PAD), row - base


def extract_kernel(here, left_pos, right_pos, own_pos, trans, own, to_left, to_right,
                   buf_own, buf_left, buf_right, sems):
    slots, _, extent, _ = own.shape
    rows, cols = trans.shape[1:]
    tall = extent + PAD
    slack = cols + 2 * RIM - extent
    jobs = (
        (left_pos, buf_left, 0, RIM),
        (right_pos, buf_right, cols - RIM, RIM),
        (own_pos, buf_own, 0, cols),
    )

    def copy(j, s):
        pos, buf, start, width = jobs[j]
        base, off = aligned(pos[s, 0], rows - tall)
        src = trans.at[:, pl.ds(base, tall), pl.ds(start, width)]
        return pltpu.make_async_copy(src, buf.at[s], sems.at[j, s]), off

    for j in range(3):
        for s in range(slots):
            copy(j, s)[0].start()

    def columns(width):
        return lax.broadcasted_iota(jnp.int32, (extent, width), 1)

    def load(j, s, p, off, turn):
        value = pltpu.roll(jobs[j][1][s, p], (tall - off) % tall, 0)[:extent]
        return pltpu.roll(value, turn, 1)

    def for_left(s, carry):
        one, off = copy(0, s)
        one.wait()
        short = slack - left_pos[s, 1]
        at = columns(RIM) - short
        good = (at >= 0) & (at + 1 <= left_pos[slots, 1])
        for p in range(2):
            value = load(0, s, p, off, short % RIM)
            to_left[s, p] = jnp.where(good, value, 0.0)
        return carry

    def for_right(s, carry):
        one, off = copy(1, s)
        one.wait()
        col = right_pos[s, 1]
        at = columns(RIM) + col
        good = (at < RIM) & (RIM - at <= right_pos[slots, 0])
        for p in range(2):
            value = load(1, s, p, off, (cols - col) % RIM)
            to_right[s, p] = jnp.where(good, value, 0.0)
        return carry

    def for_own(s, carry):
        one, off = copy(2, s)
        one.wait()
        col = own_pos[s, 1]
        at = columns(extent) + col
        middle = (at >= RIM) & (at < RIM + cols)
        left_ok = (here[0] > 0) & (at < RIM) & (RIM - at <= own_pos[slots, 0])
        right_ok = (here[0] < here[1] - 1) & (at >= RIM + cols) & (
            at - RIM - cols + 1 <= own_pos[slots, 1])
        rim = left_ok | right_ok
        for p in range(2):
            value = load(2, s, p, off, (cols + RIM - col) % cols)
            out = jnp.where(rim, 0.0, 1.0 - p)
            own[s, p] = jnp.where(middle, value, out)
        return carry

    lax.fori_loop(0, slots, for_left, 0)
    lax.fori_loop(0, slots, for_right, 0)
    lax.fori_loop(0, slots, for_own, 0)


def gather_kernel(left_pos, right_pos, own_pos, contrib, from_left, from_right, out):
    slots, _, extent, _ = contrib.shape
    rows, cols = out.shape[1:]
    tall = extent + PAD
    slack = cols + 2 * RIM - extent
    out[...] = jnp.zeros(out.shape, out.dtype)

    def columns(width):
        return lax.broadcasted_iota(jnp.int32, (extent, width), 1)

    def add(source, s, pos, good, turn, start, width):
        base, off = aligned(pos[s, 0], rows - tall)
        for p in range(2):
            value = jnp.where(good, pltpu.roll(source[s, p], turn, 1), 0.0)
            value = jnp.concatenate([value, jnp.zeros((PAD, width), jnp.float32)], axis=0)
            value = pltpu.roll(value, off, 0)
            out[p, pl.ds(base, tall), pl.ds(start, width)] += value

    def body(s, carry):
        col = own_pos[s, 1]
        at = columns(cols) + RIM - col
        good = (at >= 0) & (at < extent)
        add(contrib, s, own_pos, good, (col + cols - RIM) % cols, 0, cols)
        short = slack - left_pos[s, 1]
        at = columns(RIM)
        good = (at + short < RIM) & (at + 1 <= left_pos[slots, 1])
        add(from_left, s, left_pos, good, (cols - short) % RIM, 0, RIM)
        col = right_pos[s, 1]
        good = (at >= col) & (RIM - at <= right_pos[slots, 0])
        add(from_right, s, right_pos, good, col % RIM, cols - RIM, RIM)
        return carry

    lax.fori_loop(0, slots, body, 0)


def pipeline_kernel(sections, tiles, live, to_left, to_right, own, probe, phase_kernel, measured,
                    fwd_hi, fwd_lo, inv_hi, inv_lo, adjoint, contrib, from_left, from_right,
                    windows, left_rim, right_rim, got_left, got_right,
                    arrived, leaving, backed, left_f, left_i, right_f, right_i,
                    tall_b, wide_b, spectrum, send_f, recv_f, send_b, recv_b,
                    send_rim, recv_rim, send_got, recv_got):
    g = lax.axis_index("cuts")
    t = lax.axis_index("tile")
    last = sections - 1
    end = tiles - 1
    slots, _, extent, _ = own.shape
    two = 2 * extent

    barrier = pltpu.get_barrier_semaphore()

    @pl.when(g > 0)
    def _():
        pl.semaphore_signal(barrier, inc=1, device_id={"cuts": g - 1}, device_id_type=MESH)

    @pl.when(g < last)
    def _():
        pl.semaphore_signal(barrier, inc=1, device_id={"cuts": g + 1}, device_id_type=MESH)

    @pl.when(t > 0)
    def _():
        pl.semaphore_signal(barrier, inc=1, device_id={"tile": t - 1}, device_id_type=MESH)

    @pl.when(t < end)
    def _():
        pl.semaphore_signal(barrier, inc=1, device_id={"tile": t + 1}, device_id_type=MESH)

    for table, hi, lo in ((left_f, fwd_hi, fwd_lo), (left_i, inv_hi, inv_lo)):
        table[:, :two] = hi[...]
        table[:, two : 2 * two] = hi[...]
        table[:, 2 * two :] = lo[...]
    for table, hi, lo in ((right_f, inv_hi, inv_lo), (right_i, fwd_hi, fwd_lo)):
        table[:two] = hi[...]
        table[two : 2 * two] = hi[...]
        table[2 * two :] = lo[...]

    peers = (g + last - 1) // last + 1 - g // last + (t + end - 1) // end + 1 - t // end
    pl.semaphore_wait(barrier, peers)

    def rim_copy(side, s):
        src, dst = ((to_left, right_rim), (to_right, left_rim))[side]
        return pltpu.make_async_remote_copy(
            src_ref=src.at[s], dst_ref=dst.at[s], send_sem=send_rim.at[side, s],
            recv_sem=recv_rim.at[side, s], device_id={"tile": t + (-1, 1)[side]},
            device_id_type=MESH)

    def got_copy(side, s):
        start, dst = ((0, got_right), (extent - RIM, got_left))[side]
        return pltpu.make_async_remote_copy(
            src_ref=contrib.at[s, :, :, pl.ds(start, RIM)], dst_ref=dst.at[s],
            send_sem=send_got.at[side, s], recv_sem=recv_got.at[side, s],
            device_id={"tile": t + (-1, 1)[side]}, device_id_type=MESH)

    def each(action):
        def body(s, carry):
            action(s)
            return carry

        lax.fori_loop(0, slots, body, 0)

    @pl.when(t > 0)
    def _():
        each(lambda s: rim_copy(0, s).start())

    @pl.when(t < end)
    def _():
        each(lambda s: rim_copy(1, s).start())

    @pl.when(t == 0)
    def _():
        left_rim[...] = jnp.zeros(left_rim.shape, left_rim.dtype)
        got_left[...] = jnp.zeros(got_left.shape, got_left.dtype)

    @pl.when(t == end)
    def _():
        right_rim[...] = jnp.zeros(right_rim.shape, right_rim.dtype)
        got_right[...] = jnp.zeros(got_right.shape, got_right.dtype)

    def put(ref, rows, p, value):
        hi = value.astype(jnp.bfloat16)
        lo = (value - hi.astype(jnp.float32)).astype(jnp.bfloat16)
        n = value.shape[0 if rows else 1]
        for at, part in ((0, hi), (1, lo), (2, hi)):
            place = pl.ds(at * two + p * n, n)
            if rows:
                ref[place, :] = part
            else:
                ref[:, place] = part

    def transform(left, right):
        half = jnp.dot(left[...], tall_b[...], preferred_element_type=jnp.float32)
        put(wide_b, False, 0, half[:extent])
        put(wide_b, False, 1, half[extent:])
        spectrum[...] = jnp.dot(wide_b[...], right[...], preferred_element_type=jnp.float32)

    def times_kernel(sign):
        kr, ki = phase_kernel[0], sign * phase_kernel[1]
        xr, xi = spectrum[:, :extent], spectrum[:, extent:]
        put(tall_b, True, 0, kr * xr - ki * xi)
        put(tall_b, True, 1, kr * xi + ki * xr)

    def propagate(sign):
        transform(left_f, right_f)
        times_kernel(sign)
        transform(left_i, right_i)

    def send_forward(s):
        return pltpu.make_async_remote_copy(
            src_ref=leaving.at[s], dst_ref=arrived.at[s], send_sem=send_f.at[s],
            recv_sem=recv_f.at[s], device_id={"cuts": g + 1}, device_id_type=MESH)

    def send_backward(s):
        return pltpu.make_async_remote_copy(
            src_ref=adjoint.at[s], dst_ref=backed.at[s], send_sem=send_b.at[s],
            recv_sem=recv_b.at[s], device_id={"cuts": g - 1}, device_id_type=MESH)

    def forward(s):
        @pl.when(g == 0)
        def _():
            arrived[s] = probe[...] * live[s]

        @pl.when(g > 0)
        def _():
            send_forward(s).wait_recv()

        @pl.when(t < end)
        def _():
            rim_copy(0, s).wait_recv()

        @pl.when(t > 0)
        def _():
            rim_copy(1, s).wait_recv()

        for p in range(2):
            windows[s, p, :, :RIM] = own[s, p, :, :RIM] + left_rim[s, p]
            if extent > 2 * RIM:
                windows[s, p, :, RIM : extent - RIM] = own[s, p, :, RIM : extent - RIM]
            windows[s, p, :, extent - RIM :] = own[s, p, :, extent - RIM :] + right_rim[s, p]
        wr, wi = windows[s, 0], windows[s, 1]
        xr, xi = arrived[s, 0], arrived[s, 1]
        put(tall_b, True, 0, wr * xr - wi * xi)
        put(tall_b, True, 1, wr * xi + wi * xr)
        propagate(1.0)

        @pl.when(g < last)
        def _():
            leaving[s, 0] = spectrum[:, :extent]
            leaving[s, 1] = spectrum[:, extent:]
            send_forward(s).start()

    def backward(s):
        @pl.when(g == last)
        def _():
            put(tall_b, True, 0, spectrum[:, :extent])
            put(tall_b, True, 1, spectrum[:, extent:])
            transform(left_f, right_f)
            fr, fi = spectrum[:, :extent], spectrum[:, extent:]
            residual = fr * fr + fi * fi - measured[s].astype(jnp.float32)
            put(tall_b, True, 0, fr * residual)
            put(tall_b, True, 1, fi * residual)
            transform(left_i, right_i)
            put(tall_b, True, 0, spectrum[:, :extent])
            put(tall_b, True, 1, spectrum[:, extent:])

        @pl.when(g < last)
        def _():
            send_backward(s).wait_recv()
            put(tall_b, True, 0, backed[s, 0])
            put(tall_b, True, 1, backed[s, 1])

        propagate(-1.0)
        tr, ti = spectrum[:, :extent], spectrum[:, extent:]
        wr, wi = windows[s, 0], windows[s, 1]
        br, bi = wr * tr + wi * ti, wr * ti - wi * tr

        adjoint[s, 0] = br
        adjoint[s, 1] = bi

        @pl.when(g > 0)
        def _():
            send_backward(s).start()

        xr, xi = arrived[s, 0], arrived[s, 1]
        contrib[s, 0] = xr * tr + xi * ti
        contrib[s, 1] = xr * ti - xi * tr

        @pl.when(t > 0)
        def _():
            got_copy(0, s).start()

        @pl.when(t < end)
        def _():
            got_copy(1, s).start()

    lag = 2 * (last - g)

    def step(k, carry):
        @pl.when(k < slots)
        def _():
            forward(k)

        @pl.when((k >= lag) & (k < lag + slots))
        def _():
            backward(k - lag)

        return carry

    lax.fori_loop(0, slots + 2 * last, step, 0)

    @pl.when(g < last)
    def _():
        each(lambda s: send_forward(s).wait_send())

    @pl.when(g > 0)
    def _():
        each(lambda s: send_backward(s).wait_send())

    @pl.when(t < end)
    def _():
        each(lambda s: got_copy(0, s).wait_recv())

    @pl.when(t > 0)
    def _():
        each(lambda s: got_copy(1, s).wait_recv())

    def finish(side):
        def body(s):
            rim_copy(side, s).wait_send()
            got_copy(side, s).wait_send()

        each(body)

    @pl.when(t > 0)
    def _():
        finish(0)

    @pl.when(t < end)
    def _():
        finish(1)

    from_left[...] = got_left[...]
    from_right[...] = got_right[...]


def on_device(probe_wave, transmission, kernel_phase, measured, counts, positions, widths):
    f32 = jnp.float32
    rows, cols = transmission.shape[2:]
    extent = probe_wave.shape[-1]
    slots = positions.shape[1]
    sections = lax.axis_size("cuts")
    tiles_total = lax.axis_size("tile")
    tile_at = lax.axis_index("tile")
    tall = extent + PAD
    trans = transmission[0]
    own_pos = jnp.concatenate([positions[0], widths], 0)
    right_pos = shift(own_pos, "tile", -1)
    left_pos = shift(own_pos, "tile", 1)
    here = jnp.stack([tile_at, jnp.asarray(tiles_total, tile_at.dtype)]).astype(jnp.int32)
    sds = jax.ShapeDtypeStruct
    wave = sds((slots, 2, extent, extent), f32)
    rim = sds((slots, 2, extent, RIM), f32)
    assert extent == cols and extent >= 2 * RIM

    own, to_left, to_right = pl.pallas_call(
        extract_kernel,
        out_shape=(wave, rim, rim),
        in_specs=[smem()] * 4 + [pl.BlockSpec(memory_space=pl.ANY)],
        out_specs=(vmem(), vmem(), vmem()),
        scratch_shapes=[
            pltpu.VMEM((slots, 2, tall, cols), f32),
            pltpu.VMEM((slots, 2, tall, RIM), f32),
            pltpu.VMEM((slots, 2, tall, RIM), f32),
            pltpu.SemaphoreType.DMA((3, slots)),
        ],
        compiler_params=params(),
    )(here, left_pos, right_pos, own_pos, trans)

    tables = make_tables(extent)
    phase_kernel = jnp.stack([jnp.cos(kernel_phase), jnp.sin(kernel_phase)], 0)
    live = (jnp.arange(slots, dtype=jnp.int32) < counts[0]).astype(f32)
    waves = pltpu.VMEM((slots, 2, extent, extent), f32)
    two = 2 * extent
    bf16 = jnp.bfloat16
    rims = pltpu.VMEM((slots, 2, extent, RIM), f32)
    adjoint, contrib, from_left, from_right = pl.pallas_call(
        functools.partial(pipeline_kernel, sections, tiles_total),
        out_shape=(wave, wave, rim, rim),
        in_specs=[smem()] + [vmem()] * 10,
        out_specs=(vmem(),) * 4,
        scratch_shapes=[
            waves, rims, rims, rims, rims,
            waves, waves, waves,
            pltpu.VMEM((two, 3 * two), bf16),
            pltpu.VMEM((two, 3 * two), bf16),
            pltpu.VMEM((3 * two, two), bf16),
            pltpu.VMEM((3 * two, two), bf16),
            pltpu.VMEM((3 * two, extent), bf16),
            pltpu.VMEM((extent, 3 * two), bf16),
            pltpu.VMEM((extent, two), f32),
            pltpu.SemaphoreType.DMA((slots,)),
            pltpu.SemaphoreType.DMA((slots,)),
            pltpu.SemaphoreType.DMA((slots,)),
            pltpu.SemaphoreType.DMA((slots,)),
            pltpu.SemaphoreType.DMA((2, slots)),
            pltpu.SemaphoreType.DMA((2, slots)),
            pltpu.SemaphoreType.DMA((2, slots)),
            pltpu.SemaphoreType.DMA((2, slots)),
        ],
        compiler_params=params(collective_id=0, has_side_effects=True),
    )(live, to_left, to_right, own, probe_wave, phase_kernel, measured[0], *tables)

    grad = pl.pallas_call(
        gather_kernel,
        out_shape=sds((2, rows, cols), f32),
        in_specs=[smem()] * 3 + [vmem()] * 3,
        out_specs=vmem(),
        compiler_params=params(),
    )(left_pos, right_pos, own_pos, contrib, from_left, from_right)
    return (adjoint[None, None], grad[None])


def solution(mesh):
    return jax.shard_map(
        on_device,
        mesh=mesh,
        in_specs=(
            P(),
            P("cuts", None, None, "tile"),
            P(),
            P("tile", None, None, None),
            P("tile"),
            P("tile", None, None),
            P("tile", None),
        ),
        out_specs=(P("cuts", "tile", None, None, None, None), P("cuts", None, None, "tile")),
        check_vma=False,
    )
```

```python
import functools
import math

import jax
import jax.numpy as jnp
import numpy as np
from jax import lax
from jax.experimental import pallas as pl
from jax.experimental.pallas import tpu as pltpu
from jax.sharding import PartitionSpec as P

RIM = 128
PAD = 8
MESH = pl.DeviceIdType.MESH
VMEM_LIMIT = 60 * 1024 * 1024


def params(**kw):
    return pltpu.CompilerParams(vmem_limit_bytes=VMEM_LIMIT, **kw)


def vmem():
    return pl.BlockSpec(memory_space=pltpu.VMEM)


def smem():
    return pl.BlockSpec(memory_space=pltpu.SMEM)


def shift(value, axis, by):
    count = lax.axis_size(axis)
    pairs = [(i, i + by) for i in range(count) if 0 <= i + by < count]
    return lax.ppermute(value, axis, pairs)


def make_tables(extent):
    half = extent // 2
    indices = np.arange(extent)
    angles = (indices[:, None] * indices[None, :] % extent) * (2.0 * math.pi / extent)
    cosine = (np.cos(angles) / math.sqrt(extent)).astype(np.float32)
    sine = (np.sin(angles) / math.sqrt(extent)).astype(np.float32)
    tables = []
    for parity in range(2):
        c, s = cosine[parity::2, :half], sine[parity::2, :half]
        block = np.block([[c, s], [-s, c]])
        for matrix in (block, block.T):
            hi = matrix.astype(jnp.bfloat16)
            lo = (matrix - hi.astype(np.float32)).astype(jnp.bfloat16)
            tables += [jnp.asarray(hi), jnp.asarray(lo)]
    order = np.concatenate([indices[0::2], indices[1::2]])
    sort = (order[:, None] == indices[None, :]).astype(jnp.bfloat16)
    return tables + [jnp.asarray(sort), jnp.asarray(np.ascontiguousarray(sort.T))]


def aligned(row, limit):
    base = jnp.minimum(row // PAD * PAD, limit)
    return pl.multiple_of(base, PAD), row - base


def extract_kernel(here, left_pos, right_pos, own_pos, trans, own, to_left, to_right,
                   buf_own, buf_left, buf_right, sems):
    slots, _, extent, _ = own.shape
    rows, cols = trans.shape[1:]
    tall = extent + PAD
    slack = cols + 2 * RIM - extent
    jobs = (
        (left_pos, buf_left, 0, RIM),
        (right_pos, buf_right, cols - RIM, RIM),
        (own_pos, buf_own, 0, cols),
    )

    def copy(j, s):
        pos, buf, start, width = jobs[j]
        base, off = aligned(pos[s, 0], rows - tall)
        src = trans.at[:, pl.ds(base, tall), pl.ds(start, width)]
        return pltpu.make_async_copy(src, buf.at[s], sems.at[j, s]), off

    for j in range(3):
        for s in range(slots):
            copy(j, s)[0].start()

    def columns(width):
        return lax.broadcasted_iota(jnp.int32, (extent, width), 1)

    def load(j, s, p, off, turn):
        value = pltpu.roll(jobs[j][1][s, p], (tall - off) % tall, 0)[:extent]
        return pltpu.roll(value, turn, 1)

    def for_left(s, carry):
        one, off = copy(0, s)
        one.wait()
        short = slack - left_pos[s, 1]
        at = columns(RIM) - short
        good = (at >= 0) & (at + 1 <= left_pos[slots, 1])
        for p in range(2):
            value = load(0, s, p, off, short % RIM)
            to_left[s, p] = jnp.where(good, value, 0.0)
        return carry

    def for_right(s, carry):
        one, off = copy(1, s)
        one.wait()
        col = right_pos[s, 1]
        at = columns(RIM) + col
        good = (at < RIM) & (RIM - at <= right_pos[slots, 0])
        for p in range(2):
            value = load(1, s, p, off, (cols - col) % RIM)
            to_right[s, p] = jnp.where(good, value, 0.0)
        return carry

    def for_own(s, carry):
        one, off = copy(2, s)
        one.wait()
        col = own_pos[s, 1]
        at = columns(extent) + col
        middle = (at >= RIM) & (at < RIM + cols)
        left_ok = (here[0] > 0) & (at < RIM) & (RIM - at <= own_pos[slots, 0])
        right_ok = (here[0] < here[1] - 1) & (at >= RIM + cols) & (
            at - RIM - cols + 1 <= own_pos[slots, 1])
        rim = left_ok | right_ok
        for p in range(2):
            value = load(2, s, p, off, (cols + RIM - col) % cols)
            out = jnp.where(rim, 0.0, 1.0 - p)
            own[s, p] = jnp.where(middle, value, out)
        return carry

    lax.fori_loop(0, slots, for_left, 0)
    lax.fori_loop(0, slots, for_right, 0)
    lax.fori_loop(0, slots, for_own, 0)


def gather_kernel(left_pos, right_pos, own_pos, contrib, from_left, from_right, out):
    slots, _, extent, _ = contrib.shape
    rows, cols = out.shape[1:]
    tall = extent + PAD
    slack = cols + 2 * RIM - extent
    out[...] = jnp.zeros(out.shape, out.dtype)

    def columns(width):
        return lax.broadcasted_iota(jnp.int32, (extent, width), 1)

    def add(source, s, pos, good, turn, start, width):
        base, off = aligned(pos[s, 0], rows - tall)
        for p in range(2):
            value = jnp.where(good, pltpu.roll(source[s, p], turn, 1), 0.0)
            value = jnp.concatenate([value, jnp.zeros((PAD, width), jnp.float32)], axis=0)
            value = pltpu.roll(value, off, 0)
            out[p, pl.ds(base, tall), pl.ds(start, width)] += value

    def body(s, carry):
        col = own_pos[s, 1]
        at = columns(cols) + RIM - col
        good = (at >= 0) & (at < extent)
        add(contrib, s, own_pos, good, (col + cols - RIM) % cols, 0, cols)
        short = slack - left_pos[s, 1]
        at = columns(RIM)
        good = (at + short < RIM) & (at + 1 <= left_pos[slots, 1])
        add(from_left, s, left_pos, good, (cols - short) % RIM, 0, RIM)
        col = right_pos[s, 1]
        good = (at >= col) & (RIM - at <= right_pos[slots, 0])
        add(from_right, s, right_pos, good, col % RIM, cols - RIM, RIM)
        return carry

    lax.fori_loop(0, slots, body, 0)


def pipeline_kernel(sections, tiles, live, to_left, to_right, own, probe, phase_kernel, measured,
                    ef_hi, ef_lo, ei_hi, ei_lo, of_hi, of_lo, oi_hi, oi_lo, sort, unsort, adjoint, contrib, from_left, from_right,
                    windows, left_rim, right_rim, got_left, got_right,
                    arrived, leaving, backed, lefts, rights, turn,
                    talls, wides, freq, spectrum, send_f, recv_f, send_b, recv_b,
                    send_rim, recv_rim, send_got, recv_got):
    g = lax.axis_index("cuts")
    t = lax.axis_index("tile")
    last = sections - 1
    end = tiles - 1
    slots, _, extent, _ = own.shape
    h = extent // 2

    barrier = pltpu.get_barrier_semaphore()

    @pl.when(g > 0)
    def _():
        pl.semaphore_signal(barrier, inc=1, device_id={"cuts": g - 1}, device_id_type=MESH)

    @pl.when(g < last)
    def _():
        pl.semaphore_signal(barrier, inc=1, device_id={"cuts": g + 1}, device_id_type=MESH)

    @pl.when(t > 0)
    def _():
        pl.semaphore_signal(barrier, inc=1, device_id={"tile": t - 1}, device_id_type=MESH)

    @pl.when(t < end)
    def _():
        pl.semaphore_signal(barrier, inc=1, device_id={"tile": t + 1}, device_id_type=MESH)

    peers = (g + last - 1) // last + 1 - g // last + (t + end - 1) // end + 1 - t // end
    pl.semaphore_wait(barrier, peers)

    def rim_copy(side, s):
        src, dst = ((to_left, right_rim), (to_right, left_rim))[side]
        return pltpu.make_async_remote_copy(
            src_ref=src.at[s], dst_ref=dst.at[s], send_sem=send_rim.at[side, s],
            recv_sem=recv_rim.at[side, s], device_id={"tile": t + (-1, 1)[side]},
            device_id_type=MESH)

    def got_copy(side, s):
        start, dst = ((0, got_right), (extent - RIM, got_left))[side]
        return pltpu.make_async_remote_copy(
            src_ref=contrib.at[s, :, :, pl.ds(start, RIM)], dst_ref=dst.at[s],
            send_sem=send_got.at[side, s], recv_sem=recv_got.at[side, s],
            device_id={"tile": t + (-1, 1)[side]}, device_id_type=MESH)

    def each(action):
        def body(s, carry):
            action(s)
            return carry

        lax.fori_loop(0, slots, body, 0)

    @pl.when(t > 0)
    def _():
        each(lambda s: rim_copy(0, s).start())

    @pl.when(t < end)
    def _():
        each(lambda s: rim_copy(1, s).start())

    @pl.when(t == 0)
    def _():
        left_rim[...] = jnp.zeros(left_rim.shape, left_rim.dtype)
        got_left[...] = jnp.zeros(got_left.shape, got_left.dtype)

    @pl.when(t == end)
    def _():
        right_rim[...] = jnp.zeros(right_rim.shape, right_rim.dtype)
        got_right[...] = jnp.zeros(got_right.shape, got_right.dtype)

    forms = ((ef_hi, ef_lo, ei_hi, ei_lo), (of_hi, of_lo, oi_hi, oi_lo))
    for parity in range(2):
        fh, fl, ih, il = forms[parity]
        for inverse, (lh, ll, rh, rl) in enumerate(((fh, fl, ih, il), (ih, il, fh, fl))):
            at = 2 * inverse + parity
            lefts[at, :, :extent] = lh[...]
            lefts[at, :, extent : 2 * extent] = lh[...]
            lefts[at, :, 2 * extent :] = ll[...]
            rights[at, :extent] = rh[...]
            rights[at, extent : 2 * extent] = rh[...]
            rights[at, 2 * extent :] = rl[...]

    def exact(x, y):
        return jnp.dot(x, y, preferred_element_type=jnp.float32)

    for p in range(2):
        rest = phase_kernel[p]
        total = jnp.zeros((extent, extent), jnp.float32)
        for _ in range(3):
            part = rest.astype(jnp.bfloat16)
            rest = rest - part.astype(jnp.float32)
            rows = exact(sort[...], part).astype(jnp.bfloat16)
            total += exact(rows, unsort[...])
        turn[p] = total

    def split(value):
        hi = value.astype(jnp.bfloat16)
        lo = (value - hi.astype(jnp.float32)).astype(jnp.bfloat16)
        return (hi, lo, hi)

    def put_tall(parity, p, value):
        for at, part in enumerate(split(value)):
            talls[parity, pl.ds(at * extent + p * h, h), :] = part

    def put_wide(parity, rows, p, value):
        n = value.shape[0]
        for at, part in enumerate(split(value)):
            wides[parity, pl.ds(rows, n), pl.ds(at * extent + p * h, h)] = part

    def left(at):
        return exact(lefts[at], talls[at % 2])

    def right(at):
        return exact(wides[at % 2], rights[at])

    def to_freq(pair):
        for p in range(2):
            put_tall(0, p, pair[p][:h] + pair[p][h:])
            put_tall(1, p, pair[p][:h] - pair[p][h:])
        for block in range(2):
            half = left(block)
            for p in range(2):
                value = half[p * h : (p + 1) * h]
                put_wide(0, block * h, p, value[:, :h] + value[:, h:])
                put_wide(1, block * h, p, value[:, :h] - value[:, h:])
        for parity in range(2):
            freq[parity] = right(parity)

    def from_freq():
        u, v = right(2), right(3)
        for p in range(2):
            up, vp = u[:, p * h : (p + 1) * h], v[:, p * h : (p + 1) * h]
            plus, minus = up + vp, up - vp
            for parity in range(2):
                rows = slice(parity * h, (parity + 1) * h)
                both = jnp.concatenate([plus[rows], minus[rows]], axis=1)
                put_tall(parity, p, both)
        u, v = left(2), left(3)
        for p in range(2):
            up, vp = u[p * h : (p + 1) * h], v[p * h : (p + 1) * h]
            spectrum[p, :h] = up + vp
            spectrum[p, h:] = up - vp

    def propagate(pair, sign):
        to_freq(pair)
        for parity in range(2):
            cols = slice(parity * h, (parity + 1) * h)
            kr, ki = turn[0, :, cols], sign * turn[1, :, cols]
            xr, xi = freq[parity, :, :h], freq[parity, :, h:]
            put_wide(parity, 0, 0, kr * xr - ki * xi)
            put_wide(parity, 0, 1, kr * xi + ki * xr)
        from_freq()

    def send_forward(s):
        return pltpu.make_async_remote_copy(
            src_ref=leaving.at[s], dst_ref=arrived.at[s], send_sem=send_f.at[s],
            recv_sem=recv_f.at[s], device_id={"cuts": g + 1}, device_id_type=MESH)

    def send_backward(s):
        return pltpu.make_async_remote_copy(
            src_ref=adjoint.at[s], dst_ref=backed.at[s], send_sem=send_b.at[s],
            recv_sem=recv_b.at[s], device_id={"cuts": g - 1}, device_id_type=MESH)

    def forward(s):
        @pl.when(g == 0)
        def _():
            arrived[s] = probe[...] * live[s]

        @pl.when(g > 0)
        def _():
            send_forward(s).wait_recv()

        @pl.when(t < end)
        def _():
            rim_copy(0, s).wait_recv()

        @pl.when(t > 0)
        def _():
            rim_copy(1, s).wait_recv()

        for p in range(2):
            windows[s, p, :, :RIM] = own[s, p, :, :RIM] + left_rim[s, p]
            if extent > 2 * RIM:
                windows[s, p, :, RIM : extent - RIM] = own[s, p, :, RIM : extent - RIM]
            windows[s, p, :, extent - RIM :] = own[s, p, :, extent - RIM :] + right_rim[s, p]
        wr, wi = windows[s, 0], windows[s, 1]
        xr, xi = arrived[s, 0], arrived[s, 1]
        propagate((wr * xr - wi * xi, wr * xi + wi * xr), 1.0)

        @pl.when(g < last)
        def _():
            leaving[s, 0] = spectrum[0]
            leaving[s, 1] = spectrum[1]
            send_forward(s).start()

    def backward(s):
        @pl.when(g == last)
        def _():
            seen = exact(sort[...], measured[s]).astype(jnp.bfloat16)
            seen = exact(seen, unsort[...])
            to_freq((spectrum[0], spectrum[1]))
            for parity in range(2):
                fr, fi = freq[parity, :, :h], freq[parity, :, h:]
                residual = fr * fr + fi * fi - seen[:, parity * h : (parity + 1) * h]
                put_wide(parity, 0, 0, fr * residual)
                put_wide(parity, 0, 1, fi * residual)
            from_freq()

        @pl.when(g < last)
        def _():
            send_backward(s).wait_recv()
            spectrum[0] = backed[s, 0]
            spectrum[1] = backed[s, 1]

        propagate((spectrum[0], spectrum[1]), -1.0)
        tr, ti = spectrum[0], spectrum[1]
        wr, wi = windows[s, 0], windows[s, 1]
        br, bi = wr * tr + wi * ti, wr * ti - wi * tr

        adjoint[s, 0] = br
        adjoint[s, 1] = bi

        @pl.when(g > 0)
        def _():
            send_backward(s).start()

        xr, xi = arrived[s, 0], arrived[s, 1]
        contrib[s, 0] = xr * tr + xi * ti
        contrib[s, 1] = xr * ti - xi * tr

        @pl.when(t > 0)
        def _():
            got_copy(0, s).start()

        @pl.when(t < end)
        def _():
            got_copy(1, s).start()

    lag = 2 * (last - g)

    def step(k, carry):
        @pl.when(k < slots)
        def _():
            forward(k)

        @pl.when((k >= lag) & (k < lag + slots))
        def _():
            backward(k - lag)

        return carry

    lax.fori_loop(0, slots + 2 * last, step, 0)

    @pl.when(g < last)
    def _():
        each(lambda s: send_forward(s).wait_send())

    @pl.when(g > 0)
    def _():
        each(lambda s: send_backward(s).wait_send())

    @pl.when(t < end)
    def _():
        each(lambda s: got_copy(0, s).wait_recv())

    @pl.when(t > 0)
    def _():
        each(lambda s: got_copy(1, s).wait_recv())

    def finish(side):
        def body(s):
            rim_copy(side, s).wait_send()
            got_copy(side, s).wait_send()

        each(body)

    @pl.when(t > 0)
    def _():
        finish(0)

    @pl.when(t < end)
    def _():
        finish(1)

    from_left[...] = got_left[...]
    from_right[...] = got_right[...]


def on_device(probe_wave, transmission, kernel_phase, measured, counts, positions, widths):
    f32 = jnp.float32
    rows, cols = transmission.shape[2:]
    extent = probe_wave.shape[-1]
    slots = positions.shape[1]
    sections = lax.axis_size("cuts")
    tiles_total = lax.axis_size("tile")
    tile_at = lax.axis_index("tile")
    tall = extent + PAD
    trans = transmission[0]
    own_pos = jnp.concatenate([positions[0], widths], 0)
    right_pos = shift(own_pos, "tile", -1)
    left_pos = shift(own_pos, "tile", 1)
    here = jnp.stack([tile_at, jnp.asarray(tiles_total, tile_at.dtype)]).astype(jnp.int32)
    sds = jax.ShapeDtypeStruct
    wave = sds((slots, 2, extent, extent), f32)
    rim = sds((slots, 2, extent, RIM), f32)
    assert extent == cols and extent >= 2 * RIM

    own, to_left, to_right = pl.pallas_call(
        extract_kernel,
        out_shape=(wave, rim, rim),
        in_specs=[smem()] * 4 + [pl.BlockSpec(memory_space=pl.ANY)],
        out_specs=(vmem(), vmem(), vmem()),
        scratch_shapes=[
            pltpu.VMEM((slots, 2, tall, cols), f32),
            pltpu.VMEM((slots, 2, tall, RIM), f32),
            pltpu.VMEM((slots, 2, tall, RIM), f32),
            pltpu.SemaphoreType.DMA((3, slots)),
        ],
        compiler_params=params(),
    )(here, left_pos, right_pos, own_pos, trans)

    tables = make_tables(extent)
    phase_kernel = jnp.stack([jnp.cos(kernel_phase), jnp.sin(kernel_phase)], 0)
    live = (jnp.arange(slots, dtype=jnp.int32) < counts[0]).astype(f32)
    waves = pltpu.VMEM((slots, 2, extent, extent), f32)
    bf16 = jnp.bfloat16
    rims = pltpu.VMEM((slots, 2, extent, RIM), f32)
    adjoint, contrib, from_left, from_right = pl.pallas_call(
        functools.partial(pipeline_kernel, sections, tiles_total),
        out_shape=(wave, wave, rim, rim),
        in_specs=[smem()] + [vmem()] * 16,
        out_specs=(vmem(),) * 4,
        scratch_shapes=[
            waves, rims, rims, rims, rims,
            waves, waves, waves,
            pltpu.VMEM((4, extent, 3 * extent), bf16),
            pltpu.VMEM((4, 3 * extent, extent), bf16),
            pltpu.VMEM((2, extent, extent), f32),
            pltpu.VMEM((2, 3 * extent, extent), bf16),
            pltpu.VMEM((2, extent, 3 * extent), bf16),
            pltpu.VMEM((2, extent, extent), f32),
            pltpu.VMEM((2, extent, extent), f32),
            pltpu.SemaphoreType.DMA((slots,)),
            pltpu.SemaphoreType.DMA((slots,)),
            pltpu.SemaphoreType.DMA((slots,)),
            pltpu.SemaphoreType.DMA((slots,)),
            pltpu.SemaphoreType.DMA((2, slots)),
            pltpu.SemaphoreType.DMA((2, slots)),
            pltpu.SemaphoreType.DMA((2, slots)),
            pltpu.SemaphoreType.DMA((2, slots)),
        ],
        compiler_params=params(collective_id=0, has_side_effects=True),
    )(live, to_left, to_right, own, probe_wave, phase_kernel, measured[0], *tables)

    grad = pl.pallas_call(
        gather_kernel,
        out_shape=sds((2, rows, cols), f32),
        in_specs=[smem()] * 3 + [vmem()] * 3,
        out_specs=vmem(),
        compiler_params=params(),
    )(left_pos, right_pos, own_pos, contrib, from_left, from_right)
    return (adjoint[None, None], grad[None])


def solution(mesh):
    return jax.shard_map(
        on_device,
        mesh=mesh,
        in_specs=(
            P(),
            P("cuts", None, None, "tile"),
            P(),
            P("tile", None, None, None),
            P("tile"),
            P("tile", None, None),
            P("tile", None),
        ),
        out_specs=(P("cuts", "tile", None, None, None, None), P("cuts", None, None, "tile")),
        check_vma=False,
    )
```
